8 devices in a mesh: dp: 1 (over z), row: 2 (over y), col: 2 (over x), core: 2 (over core).
Axes of the slice: x: 2, y: 2, z: 1, core: 2. Of those that a mesh axis runs over, the one named last changes fastest.
Arguments:
- x: bfloat16 [2048, 896], P(('dp', 'row', 'col', 'core'))
- route_idx: int32 [2048, 8], P(('dp', 'row', 'col', 'core'))
- gates: float32 [2048, 8], P(('dp', 'row', 'col', 'core'))
- w1: bfloat16 [384, 896, 256], P(('row', 'col', 'core'))
- w3: bfloat16 [384, 896, 256], P(('row', 'col', 'core'))
- w2: bfloat16 [384, 256, 896], P(('row', 'col', 'core'))
- dy: bfloat16 [2048, 896], P(('dp', 'row', 'col', 'core'))
Outputs:
- output 1: bfloat16 [2048, 896], P(('dp', 'row', 'col', 'core'))
- output 2: bfloat16 [2048, 896], P(('dp', 'row', 'col', 'core'))
- output 3: float32 [2048, 8], P(('dp', 'row', 'col', 'core'))
- output 4: float32 [384, 896, 256], P(('dp', 'row', 'col', 'core'))
- output 5: float32 [384, 896, 256], P(('dp', 'row', 'col', 'core'))
- output 6: float32 [384, 256, 896], P(('dp', 'row', 'col', 'core'))
All inputs are finite; a program needn't handle non-finite values.
Results may differ from the reference program's by a relative error of at most 0.0104075.
Values are sent between devices in bfloat16 or wider.
A program may use at most 1 GiB of HBM per device.

```python
import jax
import jax.numpy as jnp
from jax import lax

TOKENS_DEV = 256
DEVICES = 8
DM = 896
FH = 256
EXPERTS = 384
TOP = 8
CAP = 14
TOKENS = TOKENS_DEV * DEVICES
GROUP_CAP = DEVICES * CAP


def _routes(key):
    half_td = TOKENS_DEV // 2
    half_e = EXPERTS // 2
    kr, ks, ka, kb = jax.random.split(jax.random.fold_in(key, 7), 4)
    ranks = jax.vmap(lambda k: jax.random.permutation(k, TOKENS_DEV))(jax.random.split(kr, DEVICES))
    sigma = jax.random.permutation(ks, EXPERTS)
    sa = jax.random.randint(ka, (), 0, half_e)
    sb = jax.random.randint(kb, (), 0, EXPERTS)
    devs = jnp.arange(DEVICES)[:, None] * half_td
    js = jnp.arange(TOP)
    ra = (ranks + devs + sa)[:, :, None] + (half_e // TOP) * js
    rb = (ranks - half_td + devs + sb)[:, :, None] + (EXPERTS // TOP) * js
    res = jnp.where((ranks < half_td)[:, :, None], ra % half_e, rb % EXPERTS)
    return sigma[res].reshape(TOKENS, TOP).astype(jnp.int32)


def setup_inputs(seed: int = 0, part: int = 0) -> dict:
    kp = jax.random.fold_in(jax.random.key(seed), part)
    kx, kr, kg, kd = jax.random.split(kp, 4)
    kw = jax.random.split(jax.random.key(seed + 1), 3)
    x = jax.random.normal(kx, (TOKENS, DM), jnp.float32).astype(jnp.bfloat16)
    route_idx = _routes(kr)
    gw = jax.random.uniform(kg, (TOKENS, TOP), jnp.float32, 0.5, 1.5)
    gates = 2.0 * gw / jnp.sum(gw, axis=1, keepdims=True)
    w1 = (jax.random.normal(kw[0], (EXPERTS, DM, FH), jnp.float32) * DM ** -0.5).astype(jnp.bfloat16)
    w3 = (jax.random.normal(kw[1], (EXPERTS, DM, FH), jnp.float32) * DM ** -0.5).astype(jnp.bfloat16)
    w2 = (jax.random.normal(kw[2], (EXPERTS, FH, DM), jnp.float32) * FH ** -0.5).astype(jnp.bfloat16)
    dy = jax.random.normal(kd, (TOKENS, DM), jnp.float32).astype(jnp.bfloat16)
    return {'x': x, 'route_idx': route_idx, 'gates': gates, 'w1': w1, 'w3': w3, 'w2': w2, 'dy': dy}


def _tables(route_idx):
    n = TOKENS * TOP
    e = route_idx.reshape(n)
    order = jnp.argsort(e, stable=True)
    counts = jnp.zeros((EXPERTS,), jnp.int32).at[e].add(1)
    starts = jnp.cumsum(counts) - counts
    c = jnp.arange(GROUP_CAP)
    pick = order[jnp.minimum(starts[:, None] + c[None, :], n - 1)]
    return jnp.where(c[None, :] < counts[:, None], pick, n)


def reference(x, route_idx, gates, w1, w3, w2, dy):
    n = TOKENS * TOP
    f32 = jnp.float32
    bf = jnp.bfloat16
    g_flat = gates.reshape(n)
    slot = _tables(route_idx)

    def expert(carry, inp):
        y_acc, dx_acc, dg = carry
        sl, a1, a3, a2 = inp
        tok = sl // TOP
        xr = jnp.take(x, tok, axis=0, mode='fill', fill_value=0)
        dyr = jnp.take(dy, tok, axis=0, mode='fill', fill_value=0)
        gr = jnp.take(g_flat, sl, mode='fill', fill_value=0)
        u = jnp.dot(xr, a1, preferred_element_type=f32).astype(bf)
        v = jnp.dot(xr, a3, preferred_element_type=f32).astype(bf)
        uf = u.astype(f32)
        vf = v.astype(f32)
        act = (jax.nn.silu(uf) * vf).astype(bf)
        o = jnp.dot(act, a2, preferred_element_type=f32).astype(bf)
        y_acc = y_acc.at[tok].add(gr[:, None] * o.astype(f32), mode='drop')
        dg = dg.at[sl].set(jnp.sum(dyr.astype(f32) * o.astype(f32), axis=1), mode='drop')
        dq = (gr[:, None] * dyr.astype(f32)).astype(bf)
        da = jnp.dot(dq, a2.T, preferred_element_type=f32).astype(bf)
        dw2 = jnp.dot(act.T, dq, preferred_element_type=f32)
        sg = jax.nn.sigmoid(uf)
        du = (da.astype(f32) * vf * sg * (1 + uf * (1 - sg))).astype(bf)
        dv = (da.astype(f32) * jax.nn.silu(uf)).astype(bf)
        dw1 = jnp.dot(xr.T, du, preferred_element_type=f32)
        dw3 = jnp.dot(xr.T, dv, preferred_element_type=f32)
        dxp = (jnp.dot(du, a1.T, preferred_element_type=f32) + jnp.dot(dv, a3.T, preferred_element_type=f32)).astype(bf)
        dx_acc = dx_acc.at[tok].add(dxp.astype(f32), mode='drop')
        return (y_acc, dx_acc, dg), (dw1, dw3, dw2)

    init = (jnp.zeros((TOKENS, DM), f32), jnp.zeros((TOKENS, DM), f32), jnp.zeros((n,), f32))
    (y_acc, dx_acc, dg), (dw1, dw3, dw2) = lax.scan(expert, init, (slot, w1, w3, w2))
    return (y_acc.astype(bf), dx_acc.astype(bf), dg.reshape(TOKENS, TOP), dw1, dw3, dw2)
```

```python
import functools

import jax
import jax.numpy as jnp
from jax import lax
from jax.experimental import pallas as pl
from jax.experimental.pallas import tpu as pltpu
from jax.sharding import PartitionSpec as P

F32 = jnp.float32
BF = jnp.bfloat16
CAP = 16
GRP = 16

_T00 = (((0,), (0,)), ((), ()))
_T11 = (((1,), (1,)), ((), ()))


def _dot(a, b, dims=(((1,), (0,)), ((), ()))):
    return lax.dot_general(a, b, dims, preferred_element_type=F32)


def _prep(aux, e0, s, td, el, pos_scr, gate_scr):
    top = aux.shape[0] // 2
    ei = lax.broadcasted_iota(jnp.int32, (el, td), 0).astype(F32)
    hit = jnp.zeros((el, td), F32)
    gate = jnp.zeros((el, td), F32)
    for j in range(top):
        eq = (aux[j:j + 1, :] - e0) == ei
        hit = jnp.where(eq, 1.0, hit)
        gate = jnp.where(eq, aux[top + j:top + j + 1, :], gate)
    before = lax.broadcasted_iota(jnp.int32, (td, td), 0) < lax.broadcasted_iota(jnp.int32, (td, td), 1)
    upper = jnp.where(before, 1.0, 0.0).astype(BF)
    rank = _dot(hit.astype(BF), upper)
    pos_scr[s] = jnp.where(hit > 0.0, rank, -1.0)
    if gate_scr is not None:
        gate_scr[s] = gate


def _mask(pos_scr, s, g, td):
    ci = lax.broadcasted_iota(jnp.int32, (CAP, td), 0).astype(F32)
    pg = pos_scr[s, pl.ds(pl.multiple_of(g * GRP, GRP), GRP), :]
    return jnp.concatenate([jnp.broadcast_to(pg[k:k + 1, :], (CAP, td)) == ci for k in range(GRP)], axis=0)


def _slot_gate(mask, gate_scr, s, g, td):
    gg = gate_scr[s, pl.ds(pl.multiple_of(g * GRP, GRP), GRP), :]
    rep = jnp.concatenate([jnp.broadcast_to(gg[k:k + 1, :], (CAP, td)) for k in range(GRP)], axis=0)
    return jnp.sum(jnp.where(mask, rep, 0.0), axis=1, keepdims=True)


def _onehot(mask):
    return jnp.where(mask, 1.0, 0.0).astype(BF)


def _e0(el):
    i = (lax.axis_index('row') * lax.axis_size('col') + lax.axis_index('col')) * lax.axis_size('core') + lax.axis_index('core')
    return (i * el).astype(F32)


def _fwd_kernel(npd, td, el, aux_ref, x_ref, w1_ref, w3_ref, w2_ref, y_ref, u_ref, v_ref, xe_ref, pos_scr, gate_scr, xg, og):
    i = pl.program_id(0)
    k = i % GRP
    g = i // GRP
    dm = x_ref.shape[1]

    @pl.when(i == 0)
    def _():
        def one(s, c):
            _prep(aux_ref[s], _e0(el), s, td, el, pos_scr, gate_scr)
            y_ref[pl.ds(pl.multiple_of(s * td, td), td), :] = jnp.zeros((td, dm), F32)
            return c
        lax.fori_loop(0, npd, one, 0)

    @pl.when(k == 0)
    def _():
        def one(s, c):
            m = _onehot(_mask(pos_scr, s, g, td))
            xs = x_ref[pl.ds(pl.multiple_of(s * td, td), td), :]
            xg[:, s] = _dot(m, xs).astype(BF).reshape(GRP, CAP, dm)
            return c
        lax.fori_loop(0, npd, one, 0)

    xe = xg[k].reshape(npd * CAP, dm)
    xe_ref[0] = xe
    u = _dot(xe, w1_ref[0]).astype(BF)
    v = _dot(xe, w3_ref[0]).astype(BF)
    u_ref[0] = u
    v_ref[0] = v
    uf = u.astype(F32)
    act = (uf * jax.nn.sigmoid(uf) * v.astype(F32)).astype(BF)
    og[k] = _dot(act, w2_ref[0]).astype(BF).reshape(npd, CAP, dm)

    @pl.when(k == GRP - 1)
    def _():
        def one(s, c):
            m = _mask(pos_scr, s, g, td)
            gs = _slot_gate(m, gate_scr, s, g, td)
            hi = gs.astype(BF).astype(F32)
            mid = (gs - hi).astype(BF).astype(F32)
            lo = gs - hi - mid
            os = og[:, s].reshape(GRP * CAP, dm)
            acc = _dot(jnp.where(m, hi, 0.0).astype(BF), os, _T00)
            acc += _dot(jnp.where(m, mid, 0.0).astype(BF), os, _T00)
            acc += _dot(jnp.where(m, lo, 0.0).astype(BF), os, _T00)
            y_ref[pl.ds(pl.multiple_of(s * td, td), td), :] += acc
            return c
        lax.fori_loop(0, npd, one, 0)


def _bwd_kernel(npd, td, el, aux_ref, dy_ref, u_ref, v_ref, w1_ref, w3_ref, w2_ref,
                dx_ref, dg_ref, dw2_ref, du_ref, dv_ref, pos_scr, gate_scr, dyg, pg, gsg, dgg):
    i = pl.program_id(0)
    k = i % GRP
    g = i // GRP
    dm = dy_ref.shape[1]
    top = dg_ref.shape[1]

    @pl.when(i == 0)
    def _():
        def one(s, c):
            _prep(aux_ref[s], _e0(el), s, td, el, pos_scr, gate_scr)
            dx_ref[pl.ds(pl.multiple_of(s * td, td), td), :] = jnp.zeros((td, dm), F32)
            dg_ref[s] = jnp.zeros((top, td), F32)
            return c
        lax.fori_loop(0, npd, one, 0)

    @pl.when(k == 0)
    def _():
        def one(s, c):
            m = _mask(pos_scr, s, g, td)
            gs = _slot_gate(m, gate_scr, s, g, td)
            gsg[:, s] = jnp.broadcast_to(gs, (GRP * CAP, 128)).reshape(GRP, CAP, 128)
            dys = dy_ref[pl.ds(pl.multiple_of(s * td, td), td), :]
            dyg[:, s] = _dot(_onehot(m), dys).astype(BF).reshape(GRP, CAP, dm)
            return c
        lax.fori_loop(0, npd, one, 0)

    rows = npd * CAP
    dye = dyg[k].reshape(rows, dm).astype(F32)
    gs = gsg[k].reshape(rows, 128)
    q = (jnp.concatenate([gs] * (dm // 128), axis=1) * dye).astype(BF)
    uf = u_ref[0].astype(F32)
    vf = v_ref[0].astype(F32)
    sg = jax.nn.sigmoid(uf)
    sl = uf * sg
    act = (sl * vf).astype(BF)
    w2 = w2_ref[0]
    o = _dot(act, w2).astype(BF).astype(F32)
    dgs = jnp.sum(dye * o, axis=1, keepdims=True)
    dgg[k] = jnp.broadcast_to(dgs, (rows, 128)).reshape(npd, CAP, 128)
    da = _dot(q, w2, _T11).astype(BF).astype(F32)
    dw2_ref[0] = _dot(act, q, _T00)
    du = (da * vf * sg * (1 + uf * (1 - sg))).astype(BF)
    dv = (da * sl).astype(BF)
    du_ref[0] = du
    dv_ref[0] = dv
    p = _dot(du, w1_ref[0], _T11) + _dot(dv, w3_ref[0], _T11)
    pg[k] = p.astype(BF).reshape(npd, CAP, dm)

    @pl.when(k == GRP - 1)
    def _():
        def one(s, c):
            m = _mask(pos_scr, s, g, td)
            ps = pg[:, s].reshape(GRP * CAP, dm)
            dx_ref[pl.ds(pl.multiple_of(s * td, td), td), :] += _dot(_onehot(m), ps, _T00)
            dgr = dgg[:, s].reshape(GRP * CAP, 128)
            dgr = jnp.concatenate([dgr] * (td // 128), axis=1)
            dge = jnp.sum(jnp.where(m, dgr, 0.0).reshape(GRP, CAP, td), axis=1)
            ei = (lax.broadcasted_iota(jnp.int32, (GRP, td), 0) + g * GRP).astype(F32)
            aux = aux_ref[s]
            e0 = _e0(el)
            out = [jnp.sum(jnp.where((aux[j:j + 1, :] - e0) == ei, dge, 0.0), axis=0, keepdims=True) for j in range(top)]
            dg_ref[s] += jnp.concatenate(out, axis=0)
            return c
        lax.fori_loop(0, npd, one, 0)


def _dw_kernel(xe_ref, du_ref, dv_ref, dw1_ref, dw3_ref):
    xe = xe_ref[0]
    dw1_ref[0] = _dot(xe, du_ref[0], _T00)
    dw3_ref[0] = _dot(xe, dv_ref[0], _T00)


def _full(shape):
    n = len(shape)
    return pl.BlockSpec(shape, lambda i: (0,) * n, pipeline_mode=pl.Buffered(1))


def _per(shape):
    n = len(shape)
    return pl.BlockSpec((1,) + shape, lambda i: (i,) + (0,) * n)


def solution(mesh):
    ep = ('row', 'col', 'core')
    npd = mesh.shape['row'] * mesh.shape['col'] * mesh.shape['core']
    tspec = P(('dp',) + ep, None)
    wspec = P(ep, None, None)
    gspec = P(('dp',) + ep, None, None)

    def body(x, route_idx, gates, w1, w3, w2, dy):
        td, top = route_idx.shape
        el, dm, fh = w1.shape
        rows = npd * CAP
        aux = jnp.concatenate([route_idx.T.astype(F32), gates.T], axis=0)
        auxa = lax.all_gather(aux, ep, axis=0)
        xa = lax.all_gather(x, ep, axis=0, tiled=True)
        dya = lax.all_gather(dy, ep, axis=0, tiled=True)
        sds = jax.ShapeDtypeStruct
        meta = [pltpu.VMEM((npd, el, td), F32), pltpu.VMEM((npd, el, td), F32)]
        y, u, v, xe = pl.pallas_call(
            functools.partial(_fwd_kernel, npd, td, el),
            grid=(el,),
            in_specs=[_full((npd, 2 * top, td)), _full((npd * td, dm)), _per((dm, fh)), _per((dm, fh)), _per((fh, dm))],
            out_specs=[_full((npd * td, dm)), _per((rows, fh)), _per((rows, fh)), _per((rows, dm))],
            out_shape=[sds((npd * td, dm), F32), sds((el, rows, fh), BF), sds((el, rows, fh), BF), sds((el, rows, dm), BF)],
            scratch_shapes=meta + [pltpu.VMEM((GRP, npd, CAP, dm), BF), pltpu.VMEM((GRP, npd, CAP, dm), BF)],
            name='moe_fwd',
        )(auxa, xa, w1, w3, w2)
        dx, dg, dw2, du, dv = pl.pallas_call(
            functools.partial(_bwd_kernel, npd, td, el),
            grid=(el,),
            in_specs=[_full((npd, 2 * top, td)), _full((npd * td, dm)), _per((rows, fh)), _per((rows, fh)),
                      _per((dm, fh)), _per((dm, fh)), _per((fh, dm))],
            out_specs=[_full((npd * td, dm)), _full((npd, top, td)), _per((fh, dm)), _per((rows, fh)), _per((rows, fh))],
            out_shape=[sds((npd * td, dm), F32), sds((npd, top, td), F32), sds((el, fh, dm), F32),
                       sds((el, rows, fh), BF), sds((el, rows, fh), BF)],
            scratch_shapes=meta + [pltpu.VMEM((GRP, npd, CAP, dm), BF), pltpu.VMEM((GRP, npd, CAP, dm), BF),
                                   pltpu.VMEM((GRP, npd, CAP, 128), F32), pltpu.VMEM((GRP, npd, CAP, 128), F32)],
            name='moe_bwd',
        )(auxa, dya, u, v, w1, w3, w2)
        dw1, dw3 = pl.pallas_call(
            _dw_kernel,
            grid=(el,),
            in_specs=[_per((rows, dm)), _per((rows, fh)), _per((rows, fh))],
            out_specs=[_per((dm, fh)), _per((dm, fh))],
            out_shape=[sds((el, dm, fh), F32), sds((el, dm, fh), F32)],
            name='moe_dw',
        )(xe, du, dv)
        ys = lax.psum_scatter(y, ep, scatter_dimension=0, tiled=True).astype(BF)
        dxs = lax.psum_scatter(dx, ep, scatter_dimension=0, tiled=True).astype(BF)
        dgs = lax.psum_scatter(dg, ep, scatter_dimension=0, tiled=False)
        return ys, dxs, dgs.T, dw1, dw3, dw2

    return jax.shard_map(body, mesh=mesh, in_specs=(tspec, tspec, tspec, wspec, wspec, wspec, tspec), out_specs=(tspec, tspec, tspec, gspec, gspec, gspec), check_vma=False)
```

```python
import functools

import jax
import jax.numpy as jnp
from jax import lax
from jax.experimental import pallas as pl
from jax.experimental.pallas import tpu as pltpu
from jax.sharding import PartitionSpec as P

F32 = jnp.float32
BF = jnp.bfloat16
CAP = 16
GRP = 16
EB = 4
NS = 3

_T00 = (((0,), (0,)), ((), ()))
_T11 = (((1,), (1,)), ((), ()))


def _dot(a, b, dims=(((1,), (0,)), ((), ()))):
    return lax.dot_general(a, b, dims, preferred_element_type=F32)


def _prep(aux, e0, s, td, el, pos_scr, gate_scr):
    top = aux.shape[0] // 2
    ei = lax.broadcasted_iota(jnp.int32, (el, td), 0).astype(F32)
    hit = jnp.zeros((el, td), F32)
    gate = jnp.zeros((el, td), F32)
    for j in range(top):
        eq = (aux[j:j + 1, :] - e0) == ei
        hit = jnp.where(eq, 1.0, hit)
        gate = jnp.where(eq, aux[top + j:top + j + 1, :], gate)
    before = lax.broadcasted_iota(jnp.int32, (td, td), 0) < lax.broadcasted_iota(jnp.int32, (td, td), 1)
    upper = jnp.where(before, 1.0, 0.0).astype(BF)
    rank = _dot(hit.astype(BF), upper)
    pos_scr[s] = jnp.where(hit > 0.0, rank, -1.0)
    if gate_scr is not None:
        gate_scr[s] = gate


def _mask(pos_scr, s, g, td):
    ci = lax.broadcasted_iota(jnp.int32, (CAP, td), 0).astype(F32)
    pg = pos_scr[s, pl.ds(pl.multiple_of(g * GRP, GRP), GRP), :]
    return jnp.concatenate([jnp.broadcast_to(pg[k:k + 1, :], (CAP, td)) == ci for k in range(GRP)], axis=0)


def _slot_gate(mask, gate_scr, s, g, td):
    gg = gate_scr[s, pl.ds(pl.multiple_of(g * GRP, GRP), GRP), :]
    rep = jnp.concatenate([jnp.broadcast_to(gg[k:k + 1, :], (CAP, td)) for k in range(GRP)], axis=0)
    return jnp.sum(jnp.where(mask, rep, 0.0), axis=1, keepdims=True)


def _onehot(mask):
    return jnp.where(mask, 1.0, 0.0).astype(BF)


def _xor(a, b):
    return a + b - 2 * a * b


def _coords():
    return lax.axis_index('row'), lax.axis_index('col'), lax.axis_index('core')


def _block(r):
    row, col, core = _coords()
    return (_xor(row, r // 4) * 2 + _xor(col, r // 2 % 2)) * 2 + _xor(core, r % 2)


def _device(r):
    row, col, core = _coords()
    return {'row': _xor(row, r // 4), 'col': _xor(col, r // 2 % 2), 'core': _xor(core, r % 2)}


def _e0(el):
    return (_block(0) * el).astype(F32)


def _rows(s, td):
    return pl.ds(pl.multiple_of(s * td, td), td)


class _Gather:
    def __init__(self, own, full, send, recv, local):
        self.own, self.full, self.send, self.recv, self.local = own, full, send, recv, local
        self.h = own.shape[0] // 2
        self.sent = []

    def _half(self, b, h):
        return pl.ds(pl.multiple_of(_block(b) * (2 * self.h) + h * self.h, self.h), self.h)

    def _send(self, d, b, h):
        src = self.own.at[pl.ds(h * self.h, self.h)] if b == 0 else self.full.at[self._half(b, h)]
        c = pltpu.make_async_remote_copy(src_ref=src, dst_ref=self.full.at[self._half(b, h)], send_sem=self.send.at[len(self.sent)],
                                         recv_sem=self.recv.at[b ^ d, h], device_id=_device(d), device_id_type=pl.DeviceIdType.MESH)
        c.start()
        self.sent.append(c)

    def _wait(self, r, h):
        ref = self.full.at[self._half(r, h)]
        pltpu.make_async_remote_copy(src_ref=ref, dst_ref=ref, send_sem=self.send.at[0], recv_sem=self.recv.at[r, h],
                                     device_id=_device(0), device_id_type=pl.DeviceIdType.MESH).wait_recv()

    def start(self):
        self.mine = pltpu.make_async_copy(self.own, self.full.at[_rows(_block(0), 2 * self.h)], self.local)
        for d, h in ((2, 0), (4, 1), (2, 1), (4, 0), (1, 0), (1, 1)):
            self._send(d, 0, h)
        self.mine.start()

    def relay(self):
        self._wait(2, 0)
        self._send(4, 2, 0)
        self._wait(4, 1)
        self._send(2, 4, 1)
        self._send(1, 2, 0)
        self._send(1, 4, 1)

    def cross(self):
        self._wait(2, 1)
        self._send(1, 2, 1)
        self._wait(4, 0)
        self._send(1, 4, 0)
        self._wait(6, 0)
        self._send(1, 6, 0)
        self._wait(6, 1)
        self._send(1, 6, 1)

    def finish(self):
        self.mine.wait()
        for r in (1, 3, 5, 7):
            for h in range(2):
                self._wait(r, h)

    def drain(self):
        for c in self.sent:
            c.wait_send()


class _Weights:
    def __init__(self, hbm, ring, sem):
        self.hbm, self.ring, self.sem = hbm, ring, sem
        self.n = hbm[0].shape[0] // EB

    def _copies(self, it):
        slot = it % NS
        return [pltpu.make_async_copy(w.at[pl.ds(it % self.n * EB, EB)], r.at[slot], self.sem.at[slot, k])
                for k, (w, r) in enumerate(zip(self.hbm, self.ring))]

    def prime(self):
        for it in range(NS):
            for c in self._copies(it):
                c.start()

    def wait(self, it):
        for c in self._copies(it):
            c.wait()
        return it % NS

    def next(self, it):
        @pl.when(it + NS < 2 * self.n)
        def _():
            for c in self._copies(it + NS):
                c.start()


def _greet(relations):
    barrier = pltpu.get_barrier_semaphore()
    for r in relations:
        pl.semaphore_signal(barrier, inc=1, device_id=_device(r), device_id_type=pl.DeviceIdType.MESH)
    pl.semaphore_wait(barrier, len(relations))


def _to_partner(acc, recv, send_sem, recv_sem, q):
    n = recv.shape[1]
    return pltpu.make_async_remote_copy(src_ref=acc.at[_block(7 - 2 * q), pl.ds(0, n)], dst_ref=recv.at[q], send_sem=send_sem.at[q],
                                        recv_sem=recv_sem.at[q], device_id=_device(1), device_id_type=pl.DeviceIdType.MESH)


def _to_chip(src, recv, send_sem, recv_sem, q):
    return pltpu.make_async_remote_copy(src_ref=src.at[q], dst_ref=recv.at[q], send_sem=send_sem.at[q], recv_sem=recv_sem.at[q],
                                        device_id=_device(6 - 2 * q), device_id_type=pl.DeviceIdType.MESH)


def _main_kernel(npd, td, el, aux_ref, x_ref, dy_ref, w1_ref, w3_ref, w2_ref,
                 y_ref, dxd_ref, dxy_ref, dxx_ref, dxs_ref, xe_ref, q_ref, act_ref, du_ref, dv_ref,
                 xa, dya, aux, acc, ur, yr, dr, w1r, w3r, w2r, rg, og, uu, vv, acts, gsg, dgg, pos_scr, gate_scr,
                 sx, rx, sd, rd, sa, ra, sp, rp, sq, rq, sc, rc, lsem, wsem, xsem, qsem, asem, osem, dsem):
    dm = x_ref.shape[1]
    top = aux_ref.shape[0] // 2
    rows = npd * CAP
    ng = el // GRP
    spg = GRP // EB
    nc = npd // 2
    weights = _Weights((w1_ref, w3_ref, w2_ref), (w1r, w3r, w2r), wsem)
    me = _block(0)
    mine = pltpu.make_async_copy(aux_ref, aux.at[me], lsem.at[2])
    mine.start()
    _greet(range(1, npd))
    gx = _Gather(x_ref, xa, sx, rx, lsem.at[0])
    gd = _Gather(dy_ref, dya, sd, rd, lsem.at[1])
    asend = [pltpu.make_async_remote_copy(src_ref=aux_ref, dst_ref=aux.at[me], send_sem=sa.at[r - 1], recv_sem=ra.at[r - 1],
                                          device_id=_device(r), device_id_type=pl.DeviceIdType.MESH) for r in range(1, npd)]
    gx.start()
    for c in asend:
        c.start()
    weights.prime()
    mine.wait()
    for r in range(1, npd):
        ref = aux.at[_block(r)]
        pltpu.make_async_remote_copy(src_ref=ref, dst_ref=ref, send_sem=sa.at[0], recv_sem=ra.at[r - 1],
                                     device_id=_device(0), device_id_type=pl.DeviceIdType.MESH).wait_recv()

    def prep(s, c):
        _prep(aux[s], _e0(el), s, td, el, pos_scr, gate_scr)
        return c
    lax.fori_loop(0, npd, prep, 0)
    gx.relay()
    gd.start()
    gx.cross()
    gx.finish()

    def act_copy(it):
        return pltpu.make_async_copy(acts.at[it % 2], act_ref.at[pl.ds(it * EB, EB)], asem.at[it % 2])

    xout = [pltpu.make_async_copy(rg, xe_ref.at[pl.ds(g * GRP, GRP)], xsem.at[0]) for g in range(ng)]
    for g in range(ng):
        if g > 0:
            xout[g - 1].wait()

        def gather(s, c):
            rg[:, s] = _dot(_onehot(_mask(pos_scr, s, g, td)), xa[_rows(s, td), :]).astype(BF).reshape(GRP, CAP, dm)
            return c
        lax.fori_loop(0, npd, gather, 0)
        xout[g].start()
        if g == 1:
            gd.relay()
        if g == 2:
            gd.cross()

        def experts(k, c):
            it = g * spg + k
            slot = weights.wait(it)

            @pl.when(it >= 2)
            def _():
                act_copy(it - 2).wait()
            for b in range(EB):
                kb = k * EB + b
                xe = rg[kb].reshape(rows, dm)
                u = _dot(xe, w1r[slot, b]).astype(BF)
                v = _dot(xe, w3r[slot, b]).astype(BF)
                uu[g * GRP + kb] = u
                vv[g * GRP + kb] = v
                uf = u.astype(F32)
                act = (uf * jax.nn.sigmoid(uf) * v.astype(F32)).astype(BF)
                acts[it % 2, b] = act
                og[kb] = _dot(act, w2r[slot, b]).astype(BF).reshape(npd, CAP, dm)
            act_copy(it).start()
            weights.next(it)
            return c
        lax.fori_loop(0, spg, experts, 0)

        def combine(s):
            m = _mask(pos_scr, s, g, td)
            gs = _slot_gate(m, gate_scr, s, g, td)
            hi = gs.astype(BF).astype(F32)
            mid = (gs - hi).astype(BF).astype(F32)
            lo = gs - hi - mid
            os = og[:, s].reshape(GRP * CAP, dm)
            y = _dot(jnp.where(m, hi, 0.0).astype(BF), os, _T00)
            y += _dot(jnp.where(m, mid, 0.0).astype(BF), os, _T00)
            y += _dot(jnp.where(m, lo, 0.0).astype(BF), os, _T00)
            return y

        body = pl.ds(0, td)
        if g == 0:
            def first(s, c):
                acc[s, body] = combine(s)
                return c
            lax.fori_loop(0, npd, first, 0)
        elif g < ng - 1:
            def more(s, c):
                acc[s, body] += combine(s)
                return c
            lax.fori_loop(0, npd, more, 0)
        else:
            def other(q, c):
                acc[_block(7 - 2 * q), body] += combine(_block(7 - 2 * q))
                _to_partner(acc, ur, sp, rp, q).start()
                return c
            lax.fori_loop(0, nc, other, 0)

            def ours(q, c):
                s = _block(6 - 2 * q)
                acc[s, body] += combine(s)
                _to_partner(acc, ur, sp, rp, q).wait_recv()
                ur[q] += acc[s, body]

                @pl.when(q < nc - 1)
                def _():
                    _to_chip(ur, yr, sc, rc, q).start()
                return c
            lax.fori_loop(0, nc, ours, 0)
    n = ng * spg
    act_copy(n - 2).wait()
    act_copy(n - 1).wait()
    gd.finish()
    xout[ng - 1].wait()

    outs = []
    for g in range(ng):
        def gather_dy(s, c):
            m = _mask(pos_scr, s, g, td)
            gs = _slot_gate(m, gate_scr, s, g, td)
            gsg[:, s] = jnp.broadcast_to(gs, (GRP * CAP, 128)).reshape(GRP, CAP, 128)
            rg[:, s] = _dot(_onehot(m), dya[_rows(s, td), :]).astype(BF).reshape(GRP, CAP, dm)
            return c
        lax.fori_loop(0, npd, gather_dy, 0)

        def q_copy(k):
            return pltpu.make_async_copy(rg.at[pl.ds(k * EB, EB)], q_ref.at[pl.ds(g * GRP + k * EB, EB)], qsem.at[k])

        def experts_back(k, c):
            it = n + g * spg + k
            slot = weights.wait(it)
            for b in range(EB):
                kb = k * EB + b
                e = g * GRP + kb
                dye = rg[kb].reshape(rows, dm).astype(F32)
                gs = gsg[kb].reshape(rows, 128)
                q = (jnp.concatenate([gs] * (dm // 128), axis=1) * dye).astype(BF)
                rg[kb] = q.reshape(npd, CAP, dm)
                uf = uu[e].astype(F32)
                vf = vv[e].astype(F32)
                sg = jax.nn.sigmoid(uf)
                sl = uf * sg
                act = (sl * vf).astype(BF)
                w2 = w2r[slot, b]
                o = _dot(act, w2).astype(BF).astype(F32)
                dgs = jnp.sum(dye * o, axis=1, keepdims=True)
                dgg[kb] = jnp.broadcast_to(dgs, (rows, 128)).reshape(npd, CAP, 128)
                dact = _dot(q, w2, _T11).astype(BF).astype(F32)
                du = (dact * vf * sg * (1 + uf * (1 - sg))).astype(BF)
                dv = (dact * sl).astype(BF)
                uu[e] = du
                vv[e] = dv
                p = _dot(du, w1r[slot, b], _T11) + _dot(dv, w3r[slot, b], _T11)
                og[kb] = p.astype(BF).reshape(npd, CAP, dm)
            q_copy(k).start()
            weights.next(it)
            return c
        lax.fori_loop(0, spg, experts_back, 0)
        for k, (a, b) in enumerate(((uu, du_ref), (vv, dv_ref))):
            outs.append(pltpu.make_async_copy(a.at[pl.ds(g * GRP, GRP)], b.at[pl.ds(g * GRP, GRP)], osem.at[2 * g + k]))
            outs[-1].start()
        if g == 0:
            for q in range(nc):
                _to_partner(acc, ur, sp, rp, q).wait_send()

            def clear(s, c):
                acc[s, pl.ds(td, top), :] = jnp.zeros((top, dm), F32)
                return c
            lax.fori_loop(0, npd, clear, 0)

        def combine_back(s):
            m = _mask(pos_scr, s, g, td)
            dxs = _dot(_onehot(m), og[:, s].reshape(GRP * CAP, dm), _T00)
            dgr = dgg[:, s].reshape(GRP * CAP, 128)
            dgr = jnp.concatenate([dgr] * (td // 128), axis=1)
            dge = jnp.sum(jnp.where(m, dgr, 0.0).reshape(GRP, CAP, td), axis=1)
            ei = (lax.broadcasted_iota(jnp.int32, (GRP, td), 0) + g * GRP).astype(F32)
            a = aux[s]
            e0 = _e0(el)
            out = [jnp.sum(jnp.where((a[j:j + 1, :] - e0) == ei, dge, 0.0), axis=0, keepdims=True) for j in range(top)]
            acc[s, pl.ds(td, top), pl.ds(0, td)] += jnp.concatenate(out, axis=0)
            return dxs

        if g == 0:
            def first_back(s, c):
                acc[s, body] = combine_back(s)
                return c
            lax.fori_loop(0, npd, first_back, 0)
        elif g < ng - 1:
            def more_back(s, c):
                acc[s, body] += combine_back(s)
                return c
            lax.fori_loop(0, npd, more_back, 0)
        else:
            def other_back(q, c):
                acc[_block(7 - 2 * q), body] += combine_back(_block(7 - 2 * q))
                _to_partner(acc, dr, sq, rq, q).start()
                return c
            lax.fori_loop(0, nc, other_back, 0)

            def ours_back(q, c):
                acc[_block(6 - 2 * q), body] += combine_back(_block(6 - 2 * q))
                return c
            lax.fori_loop(0, nc, ours_back, 0)
        for k in range(spg):
            q_copy(k).wait()
    for q, out in enumerate((dxd_ref, dxy_ref, dxx_ref, dxs_ref)):
        s = _block(6 - 2 * q)
        _to_partner(acc, dr, sq, rq, q).wait_recv()
        acc[s] += dr[q]
        outs.append(pltpu.make_async_copy(acc.at[s], out, dsem.at[q]))
        outs[-1].start()
    y = ur[nc - 1]
    for q in range(nc - 1):
        _to_chip(ur, yr, sc, rc, q).wait_recv()
        y += yr[q]
    y_ref[...] = y.astype(BF)
    for q in range(nc):
        _to_partner(acc, dr, sq, rq, q).wait_send()
    for q in range(nc - 1):
        _to_chip(ur, yr, sc, rc, q).wait_send()
    for c in asend:
        c.wait_send()
    gx.drain()
    gd.drain()
    for c in outs:
        c.wait()


def _dw_kernel(xe_ref, q_ref, act_ref, du_ref, dv_ref, dw1_ref, dw3_ref, dw2_ref):
    rows, dm = act_ref.shape[1], xe_ref.shape[3]
    for b in range(EB):
        xe = xe_ref[b].reshape(rows, dm)
        dw1_ref[b] = _dot(xe, du_ref[b], _T00)
        dw3_ref[b] = _dot(xe, dv_ref[b], _T00)
        dw2_ref[b] = _dot(act_ref[b], q_ref[b].reshape(rows, dm), _T00)


def _per(shape):
    n = len(shape)
    return pl.BlockSpec((EB,) + shape, lambda i: (i,) + (0,) * n)


def solution(mesh):
    ep = ('row', 'col', 'core')
    npd = mesh.shape['row'] * mesh.shape['col'] * mesh.shape['core']
    tspec = P(('dp',) + ep, None)
    wspec = P(ep, None, None)
    gspec = P(('dp',) + ep, None, None)

    def body(x, route_idx, gates, w1, w3, w2, dy):
        td, top = route_idx.shape
        el, dm, fh = w1.shape
        rows = npd * CAP
        tp = td + top
        nc = npd // 2
        aux = jnp.concatenate([route_idx.T.astype(F32), gates.T], axis=0)
        sds = jax.ShapeDtypeStruct
        anyspec = pl.BlockSpec(memory_space=pl.ANY)
        vm = pltpu.VMEM
        dma = pltpu.SemaphoreType.DMA
        slots = vm((GRP, npd, CAP, dm), BF)
        lanes = vm((GRP, npd, CAP, 128), F32)
        hid = vm((el, rows, fh), BF)
        part = sds((tp, dm), F32)
        y, dxd, dxy, dxx, dxs, xe, q, act, du, dv = pl.pallas_call(
            functools.partial(_main_kernel, npd, td, el),
            in_specs=[anyspec] * 6,
            out_specs=[pl.BlockSpec(memory_space=vm)] + [anyspec] * 9,
            out_shape=[sds((td, dm), BF), part, part, part, part, sds((el, npd, CAP, dm), BF), sds((el, npd, CAP, dm), BF),
                       sds((el, rows, fh), BF), sds((el, rows, fh), BF), sds((el, rows, fh), BF)],
            scratch_shapes=[vm((npd * td, dm), BF), vm((npd * td, dm), BF), vm((npd, 2 * top, td), F32),
                            vm((npd, tp, dm), F32), vm((nc, td, dm), F32), vm((nc - 1, td, dm), F32), vm((nc, tp, dm), F32),
                            vm((NS, EB, dm, fh), BF), vm((NS, EB, dm, fh), BF), vm((NS, EB, fh, dm), BF),
                            slots, slots, hid, hid, vm((2, EB, rows, fh), BF), lanes, lanes,
                            vm((npd, el, td), F32), vm((npd, el, td), F32),
                            dma((14,)), dma((8, 2)), dma((14,)), dma((8, 2)), dma((7,)), dma((7,)),
                            dma((nc,)), dma((nc,)), dma((nc,)), dma((nc,)), dma((nc - 1,)), dma((nc - 1,)),
                            dma((3,)), dma((NS, 3)), dma((1,)), dma((GRP // EB,)), dma((2,)), dma((2 * (el // GRP),)), dma((nc,))],
            compiler_params=pltpu.CompilerParams(collective_id=0, has_side_effects=True, vmem_limit_bytes=67043328),
            cost_estimate=pl.CostEstimate(flops=14 * 2 * el * rows * dm * fh, bytes_accessed=200_000_000, transcendentals=0),
            name='moe_main',
        )(aux, x, dy, w1, w3, w2)
        swap = [(0, 1), (1, 0)]
        pd = lax.ppermute(dxd, ('row', 'col'), [(i, 3 - i) for i in range(4)])
        py = lax.ppermute(dxy, 'row', swap)
        px = lax.ppermute(dxx, 'col', swap)
        slotspec = _per((npd, CAP, dm))
        dw1, dw3, dw2 = pl.pallas_call(
            _dw_kernel,
            grid=(el // EB,),
            in_specs=[slotspec, slotspec] + [_per((rows, fh))] * 3,
            out_specs=[_per((dm, fh)), _per((dm, fh)), _per((fh, dm))],
            out_shape=[sds((el, dm, fh), F32), sds((el, dm, fh), F32), sds((el, fh, dm), F32)],
            cost_estimate=pl.CostEstimate(flops=3 * 2 * el * rows * dm * fh, bytes_accessed=165_000_000, transcendentals=0),
            name='moe_dw',
        )(xe, q, act, du, dv)
        dx = dxs + px + py + pd
        return y, dx[:td].astype(BF), dx[td:, :td].T, dw1, dw3, dw2

    return jax.shard_map(body, mesh=mesh, in_specs=(tspec, tspec, tspec, wspec, wspec, wspec, tspec), out_specs=(tspec, tspec, tspec, gspec, gspec, gspec), check_vma=False)
```

```python
import functools

import jax
import jax.numpy as jnp
from jax import lax
from jax.experimental import pallas as pl
from jax.experimental.pallas import tpu as pltpu
from jax.sharding import PartitionSpec as P

F32 = jnp.float32
BF = jnp.bfloat16
CAP = 16
GRP = 16
EB = 4
NS = 3

_T00 = (((0,), (0,)), ((), ()))
_T11 = (((1,), (1,)), ((), ()))


def _dot(a, b, dims=(((1,), (0,)), ((), ()))):
    return lax.dot_general(a, b, dims, preferred_element_type=F32)


def _prep(aux, e0, s, td, el, pos_scr, gate_scr):
    top = aux.shape[0] // 2
    ei = lax.broadcasted_iota(jnp.int32, (el, td), 0).astype(F32)
    hit = jnp.zeros((el, td), F32)
    gate = jnp.zeros((el, td), F32)
    for j in range(top):
        eq = (aux[j:j + 1, :] - e0) == ei
        hit = jnp.where(eq, 1.0, hit)
        gate = jnp.where(eq, aux[top + j:top + j + 1, :], gate)
    before = lax.broadcasted_iota(jnp.int32, (td, td), 0) < lax.broadcasted_iota(jnp.int32, (td, td), 1)
    upper = jnp.where(before, 1.0, 0.0).astype(BF)
    rank = _dot(hit.astype(BF), upper)
    pos_scr[s] = jnp.where(hit > 0.0, rank, -1.0)
    if gate_scr is not None:
        gate_scr[s] = gate


def _mask(pos_scr, s, g, td):
    ci = lax.broadcasted_iota(jnp.int32, (CAP, td), 0).astype(F32)
    pg = pos_scr[s, pl.ds(pl.multiple_of(g * GRP, GRP), GRP), :]
    return jnp.concatenate([jnp.broadcast_to(pg[k:k + 1, :], (CAP, td)) == ci for k in range(GRP)], axis=0)


def _slot_gate(mask, gate_scr, s, g, td):
    gg = gate_scr[s, pl.ds(pl.multiple_of(g * GRP, GRP), GRP), :]
    rep = jnp.concatenate([jnp.broadcast_to(gg[k:k + 1, :], (CAP, td)) for k in range(GRP)], axis=0)
    return jnp.sum(jnp.where(mask, rep, 0.0), axis=1, keepdims=True)


def _onehot(mask):
    return jnp.where(mask, 1.0, 0.0).astype(BF)


def _xor(a, b):
    return a + b - 2 * a * b


def _coords():
    return lax.axis_index('row'), lax.axis_index('col'), lax.axis_index('core')


def _block(r):
    row, col, core = _coords()
    return (_xor(row, r // 4) * 2 + _xor(col, r // 2 % 2)) * 2 + _xor(core, r % 2)


def _device(r):
    row, col, core = _coords()
    return {'row': _xor(row, r // 4), 'col': _xor(col, r // 2 % 2), 'core': _xor(core, r % 2)}


def _slots_of(ref, s, rows):
    return jnp.concatenate([ref[pl.ds(pl.multiple_of(k * rows + s * CAP, CAP), CAP), :] for k in range(GRP)], axis=0)


def _each(n, f, u=8):
    u = min(u, n)
    def step(i, c):
        for j in range(u):
            f(i * u + j)
        return c
    lax.fori_loop(0, n // u, step, 0)


def _e0(el):
    return (_block(0) * el).astype(F32)


def _rows(s, td):
    return pl.ds(pl.multiple_of(s * td, td), td)


class _Gather:
    def __init__(self, own, full, send, recv, local):
        self.own, self.full, self.send, self.recv, self.local = own, full, send, recv, local
        self.h = own.shape[0] // 2
        self.sent = []

    def _half(self, b, h):
        return pl.ds(pl.multiple_of(_block(b) * (2 * self.h) + h * self.h, self.h), self.h)

    def _send(self, d, b, h):
        src = self.own.at[pl.ds(h * self.h, self.h)] if b == 0 else self.full.at[self._half(b, h)]
        c = pltpu.make_async_remote_copy(src_ref=src, dst_ref=self.full.at[self._half(b, h)], send_sem=self.send.at[len(self.sent)],
                                         recv_sem=self.recv.at[b ^ d, h], device_id=_device(d), device_id_type=pl.DeviceIdType.MESH)
        c.start()
        self.sent.append(c)

    def _wait(self, r, h):
        ref = self.full.at[self._half(r, h)]
        pltpu.make_async_remote_copy(src_ref=ref, dst_ref=ref, send_sem=self.send.at[0], recv_sem=self.recv.at[r, h],
                                     device_id=_device(0), device_id_type=pl.DeviceIdType.MESH).wait_recv()

    def start(self):
        self.mine = pltpu.make_async_copy(self.own, self.full.at[_rows(_block(0), 2 * self.h)], self.local)
        for d, h in ((2, 0), (4, 1), (2, 1), (4, 0), (1, 0), (1, 1)):
            self._send(d, 0, h)
        self.mine.start()

    def relay(self):
        self._wait(2, 0)
        self._send(4, 2, 0)
        self._wait(4, 1)
        self._send(2, 4, 1)
        self._send(1, 2, 0)
        self._send(1, 4, 1)

    def cross(self):
        self._wait(2, 1)
        self._send(1, 2, 1)
        self._wait(4, 0)
        self._send(1, 4, 0)
        self._wait(6, 0)
        self._send(1, 6, 0)
        self._wait(6, 1)
        self._send(1, 6, 1)

    def finish(self):
        self.mine.wait()
        for r in (1, 3, 5, 7):
            for h in range(2):
                self._wait(r, h)

    def drain(self):
        for c in self.sent:
            c.wait_send()


class _Weights:
    def __init__(self, hbm, ring, sem):
        self.hbm, self.ring, self.sem = hbm, ring, sem
        self.n = hbm[0].shape[0] // EB

    def _copies(self, it):
        slot = it % NS
        return [pltpu.make_async_copy(w.at[pl.ds(it % self.n * EB, EB)], r.at[slot], self.sem.at[slot, k])
                for k, (w, r) in enumerate(zip(self.hbm, self.ring))]

    def prime(self):
        for it in range(NS):
            for c in self._copies(it):
                c.start()

    def wait(self, it):
        for c in self._copies(it):
            c.wait()
        return it % NS

    def next(self, it):
        @pl.when(it + NS < 2 * self.n)
        def _():
            for c in self._copies(it + NS):
                c.start()


def _greet(relations):
    barrier = pltpu.get_barrier_semaphore()
    for r in relations:
        pl.semaphore_signal(barrier, inc=1, device_id=_device(r), device_id_type=pl.DeviceIdType.MESH)
    pl.semaphore_wait(barrier, len(relations))


def _to_partner(acc, recv, send_sem, recv_sem, q):
    n = recv.shape[1]
    return pltpu.make_async_remote_copy(src_ref=acc.at[_block(7 - 2 * q), pl.ds(0, n)], dst_ref=recv.at[q], send_sem=send_sem.at[q],
                                        recv_sem=recv_sem.at[q], device_id=_device(1), device_id_type=pl.DeviceIdType.MESH)


def _to_chip(src, recv, send_sem, recv_sem, q):
    return pltpu.make_async_remote_copy(src_ref=src.at[q], dst_ref=recv.at[q], send_sem=send_sem.at[q], recv_sem=recv_sem.at[q],
                                        device_id=_device(6 - 2 * q), device_id_type=pl.DeviceIdType.MESH)


def _main_kernel(npd, td, el, aux_ref, x_ref, dy_ref, w1_ref, w3_ref, w2_ref,
                 y_ref, dxd_ref, dxy_ref, dxx_ref, dxs_ref, xe_ref, q_ref, act_ref, du_ref, dv_ref, o_ref,
                 xa, dya, aux, acc, ur, yr, dr, w1r, w3r, w2r, rg, og, uu, vv, acts, gsg, dgg, pos_scr, gate_scr,
                 sx, rx, sd, rd, sa, ra, sp, rp, sq, rq, sc, rc, lsem, wsem, xsem, qsem, asem, osem, dsem, oosem):
    dm = x_ref.shape[1]
    top = aux_ref.shape[0] // 2
    rows = npd * CAP
    ng = el // GRP
    spg = GRP // EB
    nc = npd // 2
    weights = _Weights((w1_ref, w3_ref, w2_ref), (w1r, w3r, w2r), wsem)
    me = _block(0)
    mine = pltpu.make_async_copy(aux_ref, aux.at[me], lsem.at[2])
    mine.start()
    _greet(range(1, npd))
    gx = _Gather(x_ref, xa, sx, rx, lsem.at[0])
    gd = _Gather(dy_ref, dya, sd, rd, lsem.at[1])
    asend = [pltpu.make_async_remote_copy(src_ref=aux_ref, dst_ref=aux.at[me], send_sem=sa.at[r - 1], recv_sem=ra.at[r - 1],
                                          device_id=_device(r), device_id_type=pl.DeviceIdType.MESH) for r in range(1, npd)]
    gx.start()
    for c in asend:
        c.start()
    weights.prime()
    mine.wait()
    for r in range(1, npd):
        ref = aux.at[_block(r)]
        pltpu.make_async_remote_copy(src_ref=ref, dst_ref=ref, send_sem=sa.at[0], recv_sem=ra.at[r - 1],
                                     device_id=_device(0), device_id_type=pl.DeviceIdType.MESH).wait_recv()

    def prep(s):
        _prep(aux[s], _e0(el), s, td, el, pos_scr, gate_scr)
    _each(npd, prep)
    gx.relay()
    gd.start()
    gx.cross()
    gx.finish()

    def act_copy(it):
        return pltpu.make_async_copy(acts.at[it % 2], act_ref.at[pl.ds(it * EB, EB)], asem.at[it % 2])

    xout = [pltpu.make_async_copy(rg, xe_ref.at[pl.ds(g * GRP, GRP)], xsem.at[0]) for g in range(ng)]
    oout = [pltpu.make_async_copy(og, o_ref.at[_rows(g, GRP * rows)], oosem.at[0]) for g in range(ng)]
    oin = [pltpu.make_async_copy(o_ref.at[_rows(g, GRP * rows)], xa, oosem.at[1]) for g in range(ng)]
    for g in range(ng):
        if g > 0:
            xout[g - 1].wait()

        def gather(s):
            rg[:, s] = _dot(_onehot(_mask(pos_scr, s, g, td)), xa[_rows(s, td), :]).astype(BF).reshape(GRP, CAP, dm)
        _each(npd, gather)
        xout[g].start()
        if g > 0:
            oout[g - 1].wait()
        if g == 1:
            gd.relay()
        if g == 2:
            gd.cross()

        def experts(k, c):
            it = g * spg + k
            slot = weights.wait(it)

            @pl.when(it >= 2)
            def _():
                act_copy(it - 2).wait()
            for b in range(EB):
                kb = k * EB + b
                xe = rg[kb].reshape(rows, dm)
                u = _dot(xe, w1r[slot, b]).astype(BF)
                v = _dot(xe, w3r[slot, b]).astype(BF)
                uu[g * GRP + kb] = u
                vv[g * GRP + kb] = v
                uf = u.astype(F32)
                act = (uf * jax.nn.sigmoid(uf) * v.astype(F32)).astype(BF)
                acts[it % 2, b] = act
                og[_rows(kb, rows), :] = _dot(act, w2r[slot, b]).astype(BF)
            act_copy(it).start()
            weights.next(it)
            return c
        lax.fori_loop(0, spg, experts, 0)
        oout[g].start()

        def combine(s):
            m = _mask(pos_scr, s, g, td)
            gs = _slot_gate(m, gate_scr, s, g, td)
            hi = gs.astype(BF).astype(F32)
            mid = (gs - hi).astype(BF).astype(F32)
            lo = gs - hi - mid
            os = _slots_of(og, s, rows)
            y = _dot(jnp.where(m, hi, 0.0).astype(BF), os, _T00)
            y += _dot(jnp.where(m, mid, 0.0).astype(BF), os, _T00)
            y += _dot(jnp.where(m, lo, 0.0).astype(BF), os, _T00)
            return y

        body = pl.ds(0, td)
        if g == 0:
            def first(s):
                acc[s, body] = combine(s)
            _each(npd, first)
        elif g < ng - 1:
            def more(s):
                acc[s, body] += combine(s)
            _each(npd, more)
        else:
            def other(q, c):
                acc[_block(7 - 2 * q), body] += combine(_block(7 - 2 * q))
                _to_partner(acc, ur, sp, rp, q).start()
                return c
            lax.fori_loop(0, nc, other, 0)

            def ours(q, c):
                s = _block(6 - 2 * q)
                acc[s, body] += combine(s)
                _to_partner(acc, ur, sp, rp, q).wait_recv()
                ur[q] += acc[s, body]

                @pl.when(q < nc - 1)
                def _():
                    _to_chip(ur, yr, sc, rc, q).start()
                return c
            lax.fori_loop(0, nc, ours, 0)
    n = ng * spg
    act_copy(n - 2).wait()
    act_copy(n - 1).wait()
    gd.finish()
    xout[ng - 1].wait()
    oout[ng - 1].wait()
    gx.drain()
    oin[0].start()

    outs = []
    for g in range(ng):
        def gather_dy(s):
            m = _mask(pos_scr, s, g, td)
            gs = _slot_gate(m, gate_scr, s, g, td)
            gsg[:, s] = jnp.broadcast_to(gs, (GRP * CAP, 128)).reshape(GRP, CAP, 128)
            rg[:, s] = _dot(_onehot(m), dya[_rows(s, td), :]).astype(BF).reshape(GRP, CAP, dm)
        _each(npd, gather_dy)

        def q_copy(k):
            return pltpu.make_async_copy(rg.at[pl.ds(k * EB, EB)], q_ref.at[pl.ds(g * GRP + k * EB, EB)], qsem.at[k])

        oin[g].wait()

        def experts_back(k, c):
            it = n + g * spg + k
            slot = weights.wait(it)
            for b in range(EB):
                kb = k * EB + b
                e = g * GRP + kb
                dye = rg[kb].reshape(rows, dm).astype(F32)
                gs = gsg[kb].reshape(rows, 128)
                q = (jnp.concatenate([gs] * (dm // 128), axis=1) * dye).astype(BF)
                rg[kb] = q.reshape(npd, CAP, dm)
                uf = uu[e].astype(F32)
                vf = vv[e].astype(F32)
                sg = jax.nn.sigmoid(uf)
                sl = uf * sg
                w2 = w2r[slot, b]
                o = xa[_rows(kb, rows), :].astype(F32)
                dgs = jnp.sum(dye * o, axis=1, keepdims=True)
                dgg[kb] = jnp.broadcast_to(dgs, (rows, 128)).reshape(npd, CAP, 128)
                dact = _dot(q, w2, _T11).astype(BF).astype(F32)
                du = (dact * vf * sg * (1 + uf * (1 - sg))).astype(BF)
                dv = (dact * sl).astype(BF)
                uu[e] = du
                vv[e] = dv
                p = _dot(du, w1r[slot, b], _T11) + _dot(dv, w3r[slot, b], _T11)
                og[_rows(kb, rows), :] = p.astype(BF)
            q_copy(k).start()
            weights.next(it)
            return c
        lax.fori_loop(0, spg, experts_back, 0)
        if g < ng - 1:
            oin[g + 1].start()
        for k, (a, b) in enumerate(((uu, du_ref), (vv, dv_ref))):
            outs.append(pltpu.make_async_copy(a.at[pl.ds(g * GRP, GRP)], b.at[pl.ds(g * GRP, GRP)], osem.at[2 * g + k]))
            outs[-1].start()
        if g == 0:
            for q in range(nc):
                _to_partner(acc, ur, sp, rp, q).wait_send()

            def clear(s, c):
                acc[s, pl.ds(td, top), :] = jnp.zeros((top, dm), F32)
                return c
            lax.fori_loop(0, npd, clear, 0)

        def combine_back(s):
            m = _mask(pos_scr, s, g, td)
            dxs = _dot(_onehot(m), _slots_of(og, s, rows), _T00)
            dgr = dgg[:, s].reshape(GRP * CAP, 128)
            dgr = jnp.concatenate([dgr] * (td // 128), axis=1)
            dge = jnp.sum(jnp.where(m, dgr, 0.0).reshape(GRP, CAP, td), axis=1)
            ei = (lax.broadcasted_iota(jnp.int32, (GRP, td), 0) + g * GRP).astype(F32)
            a = aux[s]
            e0 = _e0(el)
            out = [jnp.sum(jnp.where((a[j:j + 1, :] - e0) == ei, dge, 0.0), axis=0, keepdims=True) for j in range(top)]
            acc[s, pl.ds(td, top), pl.ds(0, td)] += jnp.concatenate(out, axis=0)
            return dxs

        if g == 0:
            def first_back(s):
                acc[s, body] = combine_back(s)
            _each(npd, first_back)
        elif g < ng - 1:
            def more_back(s):
                acc[s, body] += combine_back(s)
            _each(npd, more_back)
        else:
            def other_back(q, c):
                acc[_block(7 - 2 * q), body] += combine_back(_block(7 - 2 * q))
                _to_partner(acc, dr, sq, rq, q).start()
                return c
            lax.fori_loop(0, nc, other_back, 0)

            def ours_back(q):
                acc[_block(6 - 2 * q), body] += combine_back(_block(6 - 2 * q))
            _each(nc, ours_back)
        for k in range(spg):
            q_copy(k).wait()
    for q, out in enumerate((dxd_ref, dxy_ref, dxx_ref, dxs_ref)):
        s = _block(6 - 2 * q)
        _to_partner(acc, dr, sq, rq, q).wait_recv()
        acc[s] += dr[q]
        outs.append(pltpu.make_async_copy(acc.at[s], out, dsem.at[q]))
        outs[-1].start()
    y = ur[nc - 1]
    for q in range(nc - 1):
        _to_chip(ur, yr, sc, rc, q).wait_recv()
        y += yr[q]
    y_ref[...] = y.astype(BF)
    for q in range(nc):
        _to_partner(acc, dr, sq, rq, q).wait_send()
    for q in range(nc - 1):
        _to_chip(ur, yr, sc, rc, q).wait_send()
    for c in asend:
        c.wait_send()
    gd.drain()
    for c in outs:
        c.wait()


def _dw_kernel(xe_ref, q_ref, act_ref, du_ref, dv_ref, dw1_ref, dw3_ref, dw2_ref):
    rows, dm = act_ref.shape[1], xe_ref.shape[3]
    for b in range(EB):
        xe = xe_ref[b].reshape(rows, dm)
        dw1_ref[b] = _dot(xe, du_ref[b], _T00)
        dw3_ref[b] = _dot(xe, dv_ref[b], _T00)
        dw2_ref[b] = _dot(act_ref[b], q_ref[b].reshape(rows, dm), _T00)


def _per(shape):
    n = len(shape)
    return pl.BlockSpec((EB,) + shape, lambda i: (i,) + (0,) * n)


def solution(mesh):
    ep = ('row', 'col', 'core')
    npd = mesh.shape['row'] * mesh.shape['col'] * mesh.shape['core']
    tspec = P(('dp',) + ep, None)
    wspec = P(ep, None, None)
    gspec = P(('dp',) + ep, None, None)

    def body(x, route_idx, gates, w1, w3, w2, dy):
        td, top = route_idx.shape
        el, dm, fh = w1.shape
        rows = npd * CAP
        tp = td + top
        nc = npd // 2
        aux = jnp.concatenate([route_idx.T.astype(F32), gates.T], axis=0)
        sds = jax.ShapeDtypeStruct
        anyspec = pl.BlockSpec(memory_space=pl.ANY)
        vm = pltpu.VMEM
        dma = pltpu.SemaphoreType.DMA
        slots = vm((GRP, npd, CAP, dm), BF)
        lanes = vm((GRP, npd, CAP, 128), F32)
        hid = vm((el, rows, fh), BF)
        part = sds((tp, dm), F32)
        y, dxd, dxy, dxx, dxs, xe, q, act, du, dv, _ = pl.pallas_call(
            functools.partial(_main_kernel, npd, td, el),
            in_specs=[anyspec] * 6,
            out_specs=[pl.BlockSpec(memory_space=vm)] + [anyspec] * 10,
            out_shape=[sds((td, dm), BF), part, part, part, part, sds((el, npd, CAP, dm), BF), sds((el, npd, CAP, dm), BF),
                       sds((el, rows, fh), BF), sds((el, rows, fh), BF), sds((el, rows, fh), BF), sds((el * rows, dm), BF)],
            scratch_shapes=[vm((npd * td, dm), BF), vm((npd * td, dm), BF), vm((npd, 2 * top, td), F32),
                            vm((npd, tp, dm), F32), vm((nc, td, dm), F32), vm((nc - 1, td, dm), F32), vm((nc, tp, dm), F32),
                            vm((NS, EB, dm, fh), BF), vm((NS, EB, dm, fh), BF), vm((NS, EB, fh, dm), BF),
                            slots, vm((GRP * rows, dm), BF), hid, hid, vm((2, EB, rows, fh), BF), lanes, lanes,
                            vm((npd, el, td), F32), vm((npd, el, td), F32),
                            dma((14,)), dma((8, 2)), dma((14,)), dma((8, 2)), dma((7,)), dma((7,)),
                            dma((nc,)), dma((nc,)), dma((nc,)), dma((nc,)), dma((nc - 1,)), dma((nc - 1,)),
                            dma((3,)), dma((NS, 3)), dma((1,)), dma((GRP // EB,)), dma((2,)), dma((2 * (el // GRP),)), dma((nc,)), dma((2,))],
            compiler_params=pltpu.CompilerParams(collective_id=0, has_side_effects=True, vmem_limit_bytes=67043328),
            cost_estimate=pl.CostEstimate(flops=14 * 2 * el * rows * dm * fh, bytes_accessed=200_000_000, transcendentals=0),
            name='moe_main',
        )(aux, x, dy, w1, w3, w2)
        swap = [(0, 1), (1, 0)]
        pd = lax.ppermute(dxd, ('row', 'col'), [(i, 3 - i) for i in range(4)])
        py = lax.ppermute(dxy, 'row', swap)
        px = lax.ppermute(dxx, 'col', swap)
        slotspec = _per((npd, CAP, dm))
        dw1, dw3, dw2 = pl.pallas_call(
            _dw_kernel,
            grid=(el // EB,),
            in_specs=[slotspec, slotspec] + [_per((rows, fh))] * 3,
            out_specs=[_per((dm, fh)), _per((dm, fh)), _per((fh, dm))],
            out_shape=[sds((el, dm, fh), F32), sds((el, dm, fh), F32), sds((el, fh, dm), F32)],
            cost_estimate=pl.CostEstimate(flops=3 * 2 * el * rows * dm * fh, bytes_accessed=165_000_000, transcendentals=0),
            name='moe_dw',
        )(xe, q, act, du, dv)
        dx = dxs + px + py + pd
        return y, dx[:td].astype(BF), dx[td:, :td].T, dw1, dw3, dw2

    return jax.shard_map(body, mesh=mesh, in_specs=(tspec, tspec, tspec, wspec, wspec, wspec, tspec), out_specs=(tspec, tspec, tspec, gspec, gspec, gspec), check_vma=False)
```

```python
import functools

import jax
import jax.numpy as jnp
from jax import lax
from jax.experimental import pallas as pl
from jax.experimental.pallas import tpu as pltpu
from jax.sharding import PartitionSpec as P

F32 = jnp.float32
BF = jnp.bfloat16
CAP = 16
GRP = 16
EB = 4
NS = 3

_T00 = (((0,), (0,)), ((), ()))
_T11 = (((1,), (1,)), ((), ()))


def _dot(a, b, dims=(((1,), (0,)), ((), ()))):
    return lax.dot_general(a, b, dims, preferred_element_type=F32)


def _prep(aux, e0, s, td, el, pos_scr, gate_scr):
    top = aux.shape[0] // 2
    ei = lax.broadcasted_iota(jnp.int32, (el, td), 0).astype(F32)
    hit = jnp.zeros((el, td), F32)
    gate = jnp.zeros((el, td), F32)
    for j in range(top):
        eq = (aux[j:j + 1, :] - e0) == ei
        hit = jnp.where(eq, 1.0, hit)
        gate = jnp.where(eq, aux[top + j:top + j + 1, :], gate)
    before = lax.broadcasted_iota(jnp.int32, (td, td), 0) < lax.broadcasted_iota(jnp.int32, (td, td), 1)
    upper = jnp.where(before, 1.0, 0.0).astype(BF)
    rank = _dot(hit.astype(BF), upper)
    pos_scr[s] = jnp.where(hit > 0.0, rank, -1.0)
    if gate_scr is not None:
        gate_scr[s] = gate


def _mask(pos_scr, s, g, td):
    ci = lax.broadcasted_iota(jnp.int32, (CAP, td), 0).astype(F32)
    pg = pos_scr[s, pl.ds(pl.multiple_of(g * GRP, GRP), GRP), :]
    return jnp.concatenate([jnp.broadcast_to(pg[k:k + 1, :], (CAP, td)) == ci for k in range(GRP)], axis=0)


def _slot_gate(mask, gate_scr, s, g, td):
    gg = gate_scr[s, pl.ds(pl.multiple_of(g * GRP, GRP), GRP), :]
    rep = jnp.concatenate([jnp.broadcast_to(gg[k:k + 1, :], (CAP, td)) for k in range(GRP)], axis=0)
    return jnp.sum(jnp.where(mask, rep, 0.0), axis=1, keepdims=True)


def _onehot(mask):
    return jnp.where(mask, 1.0, 0.0).astype(BF)


def _xor(a, b):
    return a + b - 2 * a * b


def _coords():
    return lax.axis_index('row'), lax.axis_index('col'), lax.axis_index('core')


def _block(r):
    row, col, core = _coords()
    return (_xor(row, r // 4) * 2 + _xor(col, r // 2 % 2)) * 2 + _xor(core, r % 2)


def _device(r):
    row, col, core = _coords()
    return {'row': _xor(row, r // 4), 'col': _xor(col, r // 2 % 2), 'core': _xor(core, r % 2)}


def _slots_of(ref, s, rows):
    return jnp.concatenate([ref[pl.ds(pl.multiple_of(k * rows + s * CAP, CAP), CAP), :] for k in range(GRP)], axis=0)


def _each(n, f, u=8):
    u = min(u, n)
    def step(i, c):
        for j in range(u):
            f(i * u + j)
        return c
    lax.fori_loop(0, n // u, step, 0)


def _e0(el):
    return (_block(0) * el).astype(F32)


def _rows(s, td):
    return pl.ds(pl.multiple_of(s * td, td), td)


class _Gather:
    def __init__(self, own, full, send, recv, local):
        self.own, self.full, self.send, self.recv, self.local = own, full, send, recv, local
        self.h = own.shape[0] // 2
        self.sent = []

    def _half(self, b, h):
        return pl.ds(pl.multiple_of(_block(b) * (2 * self.h) + h * self.h, self.h), self.h)

    def _send(self, d, b, h):
        src = self.own.at[pl.ds(h * self.h, self.h)] if b == 0 else self.full.at[self._half(b, h)]
        c = pltpu.make_async_remote_copy(src_ref=src, dst_ref=self.full.at[self._half(b, h)], send_sem=self.send.at[len(self.sent)],
                                         recv_sem=self.recv.at[b ^ d, h], device_id=_device(d), device_id_type=pl.DeviceIdType.MESH)
        c.start()
        self.sent.append(c)

    def _wait(self, r, h):
        ref = self.full.at[self._half(r, h)]
        pltpu.make_async_remote_copy(src_ref=ref, dst_ref=ref, send_sem=self.send.at[0], recv_sem=self.recv.at[r, h],
                                     device_id=_device(0), device_id_type=pl.DeviceIdType.MESH).wait_recv()

    def start(self):
        self.mine = pltpu.make_async_copy(self.own, self.full.at[_rows(_block(0), 2 * self.h)], self.local)
        for d, h in ((2, 0), (4, 1), (2, 1), (4, 0), (1, 0), (1, 1)):
            self._send(d, 0, h)
        self.mine.start()

    def relay(self):
        self._wait(2, 0)
        self._send(4, 2, 0)
        self._wait(4, 1)
        self._send(2, 4, 1)
        self._send(1, 2, 0)
        self._send(1, 4, 1)

    def cross(self):
        self._wait(2, 1)
        self._send(1, 2, 1)
        self._wait(4, 0)
        self._send(1, 4, 0)
        self._wait(6, 0)
        self._send(1, 6, 0)
        self._wait(6, 1)
        self._send(1, 6, 1)

    def finish(self):
        self.mine.wait()
        for r in (1, 3, 5, 7):
            for h in range(2):
                self._wait(r, h)

    def drain(self):
        for c in self.sent:
            c.wait_send()


class _Weights:
    def __init__(self, hbm, ring, sem):
        self.hbm, self.ring, self.sem = hbm, ring, sem
        self.n = hbm[0].shape[0] // EB

    def _copies(self, it):
        slot = it % NS
        return [pltpu.make_async_copy(w.at[pl.ds(it % self.n * EB, EB)], r.at[slot], self.sem.at[slot, k])
                for k, (w, r) in enumerate(zip(self.hbm, self.ring))]

    def prime(self):
        for it in range(NS):
            for c in self._copies(it):
                c.start()

    def wait(self, it):
        for c in self._copies(it):
            c.wait()
        return it % NS

    def next(self, it):
        @pl.when(it + NS < 2 * self.n)
        def _():
            for c in self._copies(it + NS):
                c.start()


def _greet(relations):
    barrier = pltpu.get_barrier_semaphore()
    for r in relations:
        pl.semaphore_signal(barrier, inc=1, device_id=_device(r), device_id_type=pl.DeviceIdType.MESH)
    pl.semaphore_wait(barrier, len(relations))


def _to_partner(acc, recv, send_sem, recv_sem, q):
    n = recv.shape[1]
    return pltpu.make_async_remote_copy(src_ref=acc.at[_block(7 - 2 * q), pl.ds(0, n)], dst_ref=recv.at[q], send_sem=send_sem.at[q],
                                        recv_sem=recv_sem.at[q], device_id=_device(1), device_id_type=pl.DeviceIdType.MESH)


def _to_chip(src, recv, send_sem, recv_sem, q):
    return pltpu.make_async_remote_copy(src_ref=src.at[q], dst_ref=recv.at[q], send_sem=send_sem.at[q], recv_sem=recv_sem.at[q],
                                        device_id=_device(6 - 2 * q), device_id_type=pl.DeviceIdType.MESH)


def _main_kernel(npd, td, el, aux_ref, x_ref, dy_ref, w1_ref, w3_ref, w2_ref,
                 y_ref, dxd_ref, dxy_ref, dxx_ref, dxs_ref, xe_ref, q_ref, act_ref, du_ref, dv_ref, o_ref,
                 xa, dya, aux, acc, ur, yr, dr, w1r, w3r, w2r, rg, og, uu, vv, acts, gsg, dgg, pos_scr, gate_scr,
                 sx, rx, sd, rd, sa, ra, sp, rp, sq, rq, sc, rc, lsem, wsem, xsem, qsem, asem, osem, dsem, oosem):
    dm = x_ref.shape[1]
    top = aux_ref.shape[0] // 2
    rows = npd * CAP
    ng = el // GRP
    spg = GRP // EB
    nc = npd // 2
    weights = _Weights((w1_ref, w3_ref, w2_ref), (w1r, w3r, w2r), wsem)
    me = _block(0)
    mine = pltpu.make_async_copy(aux_ref, aux.at[me], lsem.at[2])
    mine.start()
    _greet(range(1, npd))
    gx = _Gather(x_ref, xa, sx, rx, lsem.at[0])
    gd = _Gather(dy_ref, dya, sd, rd, lsem.at[1])
    asend = [pltpu.make_async_remote_copy(src_ref=aux_ref, dst_ref=aux.at[me], send_sem=sa.at[r - 1], recv_sem=ra.at[r - 1],
                                          device_id=_device(r), device_id_type=pl.DeviceIdType.MESH) for r in range(1, npd)]
    gx.start()
    for c in asend:
        c.start()
    weights.prime()
    mine.wait()
    for r in range(1, npd):
        ref = aux.at[_block(r)]
        pltpu.make_async_remote_copy(src_ref=ref, dst_ref=ref, send_sem=sa.at[0], recv_sem=ra.at[r - 1],
                                     device_id=_device(0), device_id_type=pl.DeviceIdType.MESH).wait_recv()

    def prep(s):
        _prep(aux[s], _e0(el), s, td, el, pos_scr, gate_scr)
    _each(npd, prep)
    gx.relay()
    gd.start()
    gx.cross()
    gx.finish()

    def act_copy(it):
        return pltpu.make_async_copy(acts.at[it % 2], act_ref.at[pl.ds(it * EB, EB)], asem.at[it % 2])

    xout = [pltpu.make_async_copy(rg, xe_ref.at[pl.ds(g * GRP, GRP)], xsem.at[0]) for g in range(ng)]
    oout = [pltpu.make_async_copy(og, o_ref.at[_rows(g, GRP * rows)], oosem.at[0]) for g in range(ng)]
    oin = [pltpu.make_async_copy(o_ref.at[_rows(g, GRP * rows)], xa, oosem.at[1]) for g in range(ng)]
    for g in range(ng):
        if g > 0:
            xout[g - 1].wait()

        def gather(s):
            rg[:, s] = _dot(_onehot(_mask(pos_scr, s, g, td)), xa[_rows(s, td), :]).astype(BF).reshape(GRP, CAP, dm)
        _each(npd, gather)
        xout[g].start()
        if g > 0:
            oout[g - 1].wait()
        if g == 1:
            gd.relay()
        if g == 2:
            gd.cross()

        def experts(k, c):
            it = g * spg + k
            slot = weights.wait(it)

            @pl.when(it >= 2)
            def _():
                act_copy(it - 2).wait()
            for b in range(EB):
                xe = rg[k * EB + b].reshape(rows, dm)
                uu[it * EB + b] = _dot(xe, w1r[slot, b]).astype(BF)
                vv[it * EB + b] = _dot(xe, w3r[slot, b]).astype(BF)
            for b in range(EB):
                uf = uu[it * EB + b].astype(F32)
                acts[it % 2, b] = (uf * jax.nn.sigmoid(uf) * vv[it * EB + b].astype(F32)).astype(BF)
            for b in range(EB):
                og[_rows(k * EB + b, rows), :] = _dot(acts[it % 2, b], w2r[slot, b]).astype(BF)
            act_copy(it).start()
            weights.next(it)
            return c
        lax.fori_loop(0, spg, experts, 0)
        oout[g].start()

        def combine(s):
            m = _mask(pos_scr, s, g, td)
            gs = _slot_gate(m, gate_scr, s, g, td)
            hi = gs.astype(BF).astype(F32)
            mid = (gs - hi).astype(BF).astype(F32)
            lo = gs - hi - mid
            os = _slots_of(og, s, rows)
            y = _dot(jnp.where(m, hi, 0.0).astype(BF), os, _T00)
            y += _dot(jnp.where(m, mid, 0.0).astype(BF), os, _T00)
            y += _dot(jnp.where(m, lo, 0.0).astype(BF), os, _T00)
            return y

        body = pl.ds(0, td)
        if g == 0:
            def first(s):
                acc[s, body] = combine(s)
            _each(npd, first)
        elif g < ng - 1:
            def more(s):
                acc[s, body] += combine(s)
            _each(npd, more)
        else:
            def other(q, c):
                acc[_block(7 - 2 * q), body] += combine(_block(7 - 2 * q))
                _to_partner(acc, ur, sp, rp, q).start()
                return c
            lax.fori_loop(0, nc, other, 0)

            def ours(q, c):
                s = _block(6 - 2 * q)
                acc[s, body] += combine(s)
                _to_partner(acc, ur, sp, rp, q).wait_recv()
                ur[q] += acc[s, body]

                @pl.when(q < nc - 1)
                def _():
                    _to_chip(ur, yr, sc, rc, q).start()
                return c
            lax.fori_loop(0, nc, ours, 0)
    n = ng * spg
    act_copy(n - 2).wait()
    act_copy(n - 1).wait()
    gd.finish()
    xout[ng - 1].wait()
    oout[ng - 1].wait()
    gx.drain()
    oin[0].start()

    outs = []
    for g in range(ng):
        def gather_dy(s):
            m = _mask(pos_scr, s, g, td)
            gs = _slot_gate(m, gate_scr, s, g, td)
            gsg[:, s] = jnp.broadcast_to(gs, (GRP * CAP, 128)).reshape(GRP, CAP, 128)
            rg[:, s] = _dot(_onehot(m), dya[_rows(s, td), :]).astype(BF).reshape(GRP, CAP, dm)
        _each(npd, gather_dy)

        def q_copy(k):
            return pltpu.make_async_copy(rg.at[pl.ds(k * EB, EB)], q_ref.at[pl.ds(g * GRP + k * EB, EB)], qsem.at[k])

        oin[g].wait()

        def experts_back(k, c):
            it = n + g * spg + k
            slot = weights.wait(it)
            for b in range(EB):
                kb = k * EB + b
                dye = rg[kb].reshape(rows, dm).astype(F32)
                gs = gsg[kb].reshape(rows, 128)
                rg[kb] = (jnp.concatenate([gs] * (dm // 128), axis=1) * dye).astype(BF).reshape(npd, CAP, dm)
                dgs = jnp.sum(dye * xa[_rows(kb, rows), :].astype(F32), axis=1, keepdims=True)
                dgg[kb] = jnp.broadcast_to(dgs, (rows, 128)).reshape(npd, CAP, 128)
            for b in range(EB):
                kb = k * EB + b
                e = g * GRP + kb
                dact = _dot(rg[kb].reshape(rows, dm), w2r[slot, b], _T11).astype(BF).astype(F32)
                uf = uu[e].astype(F32)
                vf = vv[e].astype(F32)
                sg = jax.nn.sigmoid(uf)
                uu[e] = (dact * vf * sg * (1 + uf * (1 - sg))).astype(BF)
                vv[e] = (dact * (uf * sg)).astype(BF)
            for b in range(EB):
                kb = k * EB + b
                e = g * GRP + kb
                p = _dot(uu[e], w1r[slot, b], _T11) + _dot(vv[e], w3r[slot, b], _T11)
                og[_rows(kb, rows), :] = p.astype(BF)
            q_copy(k).start()
            weights.next(it)
            return c
        lax.fori_loop(0, spg, experts_back, 0)
        if g < ng - 1:
            oin[g + 1].start()
        for k, (a, b) in enumerate(((uu, du_ref), (vv, dv_ref))):
            outs.append(pltpu.make_async_copy(a.at[pl.ds(g * GRP, GRP)], b.at[pl.ds(g * GRP, GRP)], osem.at[2 * g + k]))
            outs[-1].start()
        if g == 0:
            for q in range(nc):
                _to_partner(acc, ur, sp, rp, q).wait_send()

            def clear(s, c):
                acc[s, pl.ds(td, top), :] = jnp.zeros((top, dm), F32)
                return c
            lax.fori_loop(0, npd, clear, 0)

        def combine_back(s):
            m = _mask(pos_scr, s, g, td)
            dxs = _dot(_onehot(m), _slots_of(og, s, rows), _T00)
            dgr = dgg[:, s].reshape(GRP * CAP, 128)
            dgr = jnp.concatenate([dgr] * (td // 128), axis=1)
            dge = jnp.sum(jnp.where(m, dgr, 0.0).reshape(GRP, CAP, td), axis=1)
            ei = (lax.broadcasted_iota(jnp.int32, (GRP, td), 0) + g * GRP).astype(F32)
            a = aux[s]
            e0 = _e0(el)
            out = [jnp.sum(jnp.where((a[j:j + 1, :] - e0) == ei, dge, 0.0), axis=0, keepdims=True) for j in range(top)]
            acc[s, pl.ds(td, top), pl.ds(0, td)] += jnp.concatenate(out, axis=0)
            return dxs

        if g == 0:
            def first_back(s):
                acc[s, body] = combine_back(s)
            _each(npd, first_back)
        elif g < ng - 1:
            def more_back(s):
                acc[s, body] += combine_back(s)
            _each(npd, more_back)
        else:
            def other_back(q, c):
                acc[_block(7 - 2 * q), body] += combine_back(_block(7 - 2 * q))
                _to_partner(acc, dr, sq, rq, q).start()
                return c
            lax.fori_loop(0, nc, other_back, 0)

            def ours_back(q):
                acc[_block(6 - 2 * q), body] += combine_back(_block(6 - 2 * q))
            _each(nc, ours_back)
        for k in range(spg):
            q_copy(k).wait()
    for q, out in enumerate((dxd_ref, dxy_ref, dxx_ref, dxs_ref)):
        s = _block(6 - 2 * q)
        _to_partner(acc, dr, sq, rq, q).wait_recv()
        acc[s] += dr[q]
        outs.append(pltpu.make_async_copy(acc.at[s], out, dsem.at[q]))
        outs[-1].start()
    y = ur[nc - 1]
    for q in range(nc - 1):
        _to_chip(ur, yr, sc, rc, q).wait_recv()
        y += yr[q]
    y_ref[...] = y.astype(BF)
    for q in range(nc):
        _to_partner(acc, dr, sq, rq, q).wait_send()
    for q in range(nc - 1):
        _to_chip(ur, yr, sc, rc, q).wait_send()
    for c in asend:
        c.wait_send()
    gd.drain()
    for c in outs:
        c.wait()


def _dw_kernel(xe_ref, q_ref, act_ref, du_ref, dv_ref, dw1_ref, dw3_ref, dw2_ref):
    rows, dm = act_ref.shape[1], xe_ref.shape[3]
    for b in range(EB):
        xe = xe_ref[b].reshape(rows, dm)
        dw1_ref[b] = _dot(xe, du_ref[b], _T00)
        dw3_ref[b] = _dot(xe, dv_ref[b], _T00)
        dw2_ref[b] = _dot(act_ref[b], q_ref[b].reshape(rows, dm), _T00)


def _per(shape):
    n = len(shape)
    return pl.BlockSpec((EB,) + shape, lambda i: (i,) + (0,) * n)


def solution(mesh):
    ep = ('row', 'col', 'core')
    npd = mesh.shape['row'] * mesh.shape['col'] * mesh.shape['core']
    tspec = P(('dp',) + ep, None)
    wspec = P(ep, None, None)
    gspec = P(('dp',) + ep, None, None)

    def body(x, route_idx, gates, w1, w3, w2, dy):
        td, top = route_idx.shape
        el, dm, fh = w1.shape
        rows = npd * CAP
        tp = td + top
        nc = npd // 2
        aux = jnp.concatenate([route_idx.T.astype(F32), gates.T], axis=0)
        sds = jax.ShapeDtypeStruct
        anyspec = pl.BlockSpec(memory_space=pl.ANY)
        vm = pltpu.VMEM
        dma = pltpu.SemaphoreType.DMA
        slots = vm((GRP, npd, CAP, dm), BF)
        lanes = vm((GRP, npd, CAP, 128), F32)
        hid = vm((el, rows, fh), BF)
        part = sds((tp, dm), F32)
        y, dxd, dxy, dxx, dxs, xe, q, act, du, dv, _ = pl.pallas_call(
            functools.partial(_main_kernel, npd, td, el),
            in_specs=[anyspec] * 6,
            out_specs=[pl.BlockSpec(memory_space=vm)] + [anyspec] * 10,
            out_shape=[sds((td, dm), BF), part, part, part, part, sds((el, npd, CAP, dm), BF), sds((el, npd, CAP, dm), BF),
                       sds((el, rows, fh), BF), sds((el, rows, fh), BF), sds((el, rows, fh), BF), sds((el * rows, dm), BF)],
            scratch_shapes=[vm((npd * td, dm), BF), vm((npd * td, dm), BF), vm((npd, 2 * top, td), F32),
                            vm((npd, tp, dm), F32), vm((nc, td, dm), F32), vm((nc - 1, td, dm), F32), vm((nc, tp, dm), F32),
                            vm((NS, EB, dm, fh), BF), vm((NS, EB, dm, fh), BF), vm((NS, EB, fh, dm), BF),
                            slots, vm((GRP * rows, dm), BF), hid, hid, vm((2, EB, rows, fh), BF), lanes, lanes,
                            vm((npd, el, td), F32), vm((npd, el, td), F32),
                            dma((14,)), dma((8, 2)), dma((14,)), dma((8, 2)), dma((7,)), dma((7,)),
                            dma((nc,)), dma((nc,)), dma((nc,)), dma((nc,)), dma((nc - 1,)), dma((nc - 1,)),
                            dma((3,)), dma((NS, 3)), dma((1,)), dma((GRP // EB,)), dma((2,)), dma((2 * (el // GRP),)), dma((nc,)), dma((2,))],
            compiler_params=pltpu.CompilerParams(collective_id=0, has_side_effects=True, vmem_limit_bytes=67043328),
            cost_estimate=pl.CostEstimate(flops=14 * 2 * el * rows * dm * fh, bytes_accessed=200_000_000, transcendentals=0),
            name='moe_main',
        )(aux, x, dy, w1, w3, w2)
        swap = [(0, 1), (1, 0)]
        pd = lax.ppermute(dxd, ('row', 'col'), [(i, 3 - i) for i in range(4)])
        py = lax.ppermute(dxy, 'row', swap)
        px = lax.ppermute(dxx, 'col', swap)
        slotspec = _per((npd, CAP, dm))
        dw1, dw3, dw2 = pl.pallas_call(
            _dw_kernel,
            grid=(el // EB,),
            in_specs=[slotspec, slotspec] + [_per((rows, fh))] * 3,
            out_specs=[_per((dm, fh)), _per((dm, fh)), _per((fh, dm))],
            out_shape=[sds((el, dm, fh), F32), sds((el, dm, fh), F32), sds((el, fh, dm), F32)],
            cost_estimate=pl.CostEstimate(flops=3 * 2 * el * rows * dm * fh, bytes_accessed=165_000_000, transcendentals=0),
            name='moe_dw',
        )(xe, q, act, du, dv)
        dx = dxs + px + py + pd
        return y, dx[:td].astype(BF), dx[td:, :td].T, dw1, dw3, dw2

    return jax.shard_map(body, mesh=mesh, in_specs=(tspec, tspec, tspec, wspec, wspec, wspec, tspec), out_specs=(tspec, tspec, tspec, gspec, gspec, gspec), check_vma=False)
```
